256 devices in a mesh: wide: 32 (over z, x), narrow: 8 (over y, core).
Axes of the slice: x: 4, y: 4, z: 8, core: 2. Of those that a mesh axis runs over, the one named last changes fastest.
Arguments:
- payload: bfloat16 [1048576, 128], P(('wide', 'narrow')), may hold values from -6 to 6
- first_key: int32 [1048576], P(('wide', 'narrow')), may hold values from 0 to 1073741823
- second_key: int32 [1048576], P(('wide', 'narrow')), may hold values from 0 to 1073741823
- live: int32 [1048576], P(('wide', 'narrow')), may hold values from 0 to 1
- first_bucket: int32 [1048576], P(('wide', 'narrow')), may hold values from 0 to 31, as said below
- second_bucket: int32 [1048576], P(('wide', 'narrow')), may hold values from 0 to 7
Outputs:
- group_mean: bfloat16 [1048576, 128], P(('wide', 'narrow'))
- duplicate_count: int32 [], replicated
The draws below stay inside these ranges and needn't reach their ends.
Inputs may be any that keep to these rules, and one draw needn't show every extreme that they name: Each device's rows name each pair (first_bucket, second_bucket) exactly 16 times; in every draw there is one bucket pair all of whose rows survive; other rows survive or not as `live` says.
All inputs are finite; a program needn't handle non-finite values.
Results may differ from the reference program's by a relative error of at most 0.001.
Values may be sent and summed in bfloat16 or wider, within the bound.
A program may use at most 64 MiB of HBM per device.

```python
import jax
import jax.numpy as jnp

COLS = 128
ROWS_DEV = 4096
GROUPS = 1024
ROWS = 1048576
N_NARROW = 8
DEVICES = 256


def layout_draw(key):
    base = jax.random.fold_in(key, 11)
    keys = jax.random.split(base, 8)
    sources = jax.random.split(keys[0], DEVICES)
    per_slot = ROWS_DEV // DEVICES
    owner = jax.vmap(lambda source_key: jax.random.permutation(source_key, ROWS_DEV) // per_slot)(sources).reshape(-1).astype(jnp.int32)
    group = jax.random.randint(keys[1], (ROWS,), 0, GROUPS)
    half_count = DEVICES * (GROUPS // 2)
    high_part = jax.random.permutation(keys[2], half_count).astype(jnp.int32)
    low_part = jax.random.randint(keys[3], (half_count,), 0, 4096)
    table_one = high_part * 4096 + low_part
    owner_base = jax.random.randint(keys[4], (DEVICES,), 0, 67108864)
    raw_first = table_one[owner * (GROUPS // 2) + group // 2]
    lowest = jnp.min(raw_first)
    highest = jnp.max(raw_first)
    first = jnp.where(raw_first == highest, 1073741823, raw_first - lowest).astype(jnp.int32)
    second = owner_base[owner] * 16 + group % 16
    keep_rate = jax.random.randint(keys[5], (DEVICES,), 150, 1025)
    hottest = jax.random.randint(keys[6], (), 0, DEVICES)
    keep_rate = jnp.where(jnp.arange(DEVICES) == hottest, 1024, keep_rate)
    alive = (jax.random.randint(keys[7], (ROWS,), 0, 1024) < keep_rate[owner]).astype(jnp.int32)
    return (owner, first, second, alive)


def draw_first_key(key, part):
    return layout_draw(key)[1].astype(jnp.int32)


def draw_second_key(key, part):
    return layout_draw(key)[2].astype(jnp.int32)


def draw_live(key, part):
    return layout_draw(key)[3].astype(jnp.int32)


def draw_first_bucket(key, part):
    return (layout_draw(key)[0] // N_NARROW).astype(jnp.int32)


def draw_second_bucket(key, part):
    return (layout_draw(key)[0] % N_NARROW).astype(jnp.int32)


def steps_of(rng, dims, shards, smallest, largest):
    factor_of, own = 1.0, jax.random.fold_in(rng, 6)
    for axis_at, shards_of in shards:
        steps = jnp.exp(jax.random.uniform(jax.random.fold_in(own, axis_at), (shards_of,), jnp.float32, smallest / len(shards), largest / len(shards)))
        factor_of = factor_of * jnp.repeat(steps, dims[axis_at] // shards_of).reshape([-1 if axis == axis_at else 1 for axis in range(len(dims))])
    return factor_of


def gaussian(own_key, dims, scale, limit, cuts=(), kind=jnp.bfloat16):
    values = scale * jax.random.normal(own_key, dims, jnp.float32)
    if cuts:
        values = values * steps_of(own_key, dims, cuts, -0.22, 0.18)
    return jnp.clip(values, -limit, limit).astype(kind)


def setup_inputs(seed: int = 0) -> dict:
    key_list = jax.random.split(jax.random.key(seed), 7)
    return {
        "payload": gaussian(key_list[0], (ROWS, COLS), 1.0, 6.0, ((0, 256),)),
        "first_key": draw_first_key(jax.random.fold_in(key_list[6], 71), 0),
        "second_key": draw_second_key(jax.random.fold_in(key_list[6], 71), 0),
        "live": draw_live(jax.random.fold_in(key_list[6], 71), 0),
        "first_bucket": draw_first_bucket(jax.random.fold_in(key_list[6], 71), 0),
        "second_bucket": draw_second_bucket(jax.random.fold_in(key_list[6], 71), 0),
    }


def reference(payload, first_key, second_key, live, first_bucket, second_bucket):
    row_total = payload.shape[0]
    position = jnp.arange(row_total, dtype=jnp.int32)
    dead = (1 - live).astype(jnp.int32)
    sort_order = jnp.lexsort((position, second_key, first_key, second_bucket, first_bucket, dead))
    fields = jnp.stack([dead, first_bucket, second_bucket, first_key, second_key], 0)[:, sort_order]
    change = jnp.any(fields[:, 1:] != fields[:, :-1], axis=0)
    starts = jnp.concatenate([jnp.ones((1,), jnp.bool_), change])
    segment = (jnp.cumsum(starts.astype(jnp.int32)) - 1).astype(jnp.int32)
    live_sorted = live[sort_order].astype(jnp.float32)
    values = payload[sort_order].astype(jnp.float32) * live_sorted[:, None]
    sums = jax.ops.segment_sum(values, segment, num_segments=row_total)
    counts = jax.ops.segment_sum(live_sorted, segment, num_segments=row_total)
    mean_sorted = sums[segment] / jnp.maximum(counts[segment], 1.0)[:, None]
    group_mean = jnp.zeros_like(mean_sorted).at[sort_order].set(mean_sorted).astype(jnp.bfloat16)
    duplicate_count = jnp.sum(live_sorted * (1.0 - starts.astype(jnp.float32))).astype(jnp.int32)
    return group_mean, duplicate_count
```

```python
import functools

import jax
import jax.numpy as jnp
from jax import lax
from jax.experimental import pallas as pl
from jax.experimental.pallas import tpu as pltpu
from jax.sharding import Mesh
from jax.sharding import PartitionSpec as P

AXES = ("z", "x", "y", "c")
MESH_ID = pl.DeviceIdType.MESH
f32, bf16, i32 = jnp.float32, jnp.bfloat16, jnp.int32
SLOT = 16
LANES = 128


def onehot(mask):
    return jnp.where(mask, 1.0, 0.0).astype(bf16)


def rows_at(start, size, align):
    return pl.ds(pl.multiple_of(start, align), size)


class Plan:
    def __init__(self, dims, chunk, block):
        self.dims = dims
        self.devices = 1
        for n in dims:
            self.devices *= n
        self.mul = 37 % self.devices
        self.mul_inverse = pow(self.mul, -1, self.devices)
        self.rows = self.devices * SLOT
        self.chunk = chunk
        self.chunks = self.rows // chunk
        self.chunk_slots = chunk // SLOT
        self.block = block
        self.row_lines = self.rows // LANES

    def partner(self, slot, sign):
        offset = lax.rem(slot * self.mul, self.devices)
        ids = []
        for n, axis in reversed(list(zip(self.dims, AXES))):
            step = lax.rem(offset, n)
            offset = offset // n
            ids.append(lax.rem(lax.axis_index(axis) + (step if sign > 0 else n - step), n))
        return tuple(reversed(ids))

    def slot_of(self, coords):
        offset = jnp.zeros_like(coords[0])
        for n, axis, at in zip(self.dims, AXES, coords):
            offset = offset * n + lax.rem(at - lax.axis_index(axis) + n, n)
        return lax.rem(offset * self.mul_inverse, self.devices)


def column_form(lines, col_ref, plan):
    turned = jnp.transpose(lines)
    for b in range(plan.row_lines):
        col_ref[pl.ds(b * LANES, LANES), :] = jnp.broadcast_to(turned[:, b : b + 1], (LANES, LANES))


def wide_line(ref, chunk_index, plan):
    n = plan.chunk // LANES
    return jnp.concatenate([ref[pl.ds(chunk_index * n + t, 1), :] for t in range(n)], axis=1)


def kernel(plan, pay_hbm, ord_ref, k1_ref, k2_ref, out_hbm, dup_ref, pay, send, recv, mean, ret, col_a, col_b,
           tag_send, tag_recv, line_a, line_b, acc, back, io_sem, tag_sems, pay_send_sem, pay_sems, ret_send_sem, ret_sems):
    dev, rows, chunk, block = plan.devices, plan.rows, plan.chunk, plan.block
    load = pltpu.make_async_copy(pay_hbm, pay, io_sem)
    load.start()
    barrier = pltpu.get_barrier_semaphore()

    def greet(slot, carry):
        pl.semaphore_signal(barrier, inc=1, device_id=plan.partner(slot, 1), device_id_type=MESH_ID)
        return carry

    lax.fori_loop(1, dev, greet, 0)

    part = lax.broadcasted_iota(i32, (8, LANES), 1) // SLOT
    sub = lax.broadcasted_iota(i32, (8, LANES), 0)
    mine = part == sub
    half = part == lax.rem(sub + 4, 8)
    for a in range(plan.row_lines):
        one = jnp.broadcast_to(k1_ref[pl.ds(a, 1), :], (8, LANES))
        two = jnp.broadcast_to(pltpu.roll(k2_ref[pl.ds(a, 1), :], LANES // 2, 1), (8, LANES))
        tag_send[pl.ds(8 * a, 8), :] = jnp.where(mine, one, two)
    column_form(ord_ref[...], col_a, plan)
    load.wait()

    deep = min(1024, rows)
    lane = lax.broadcasted_iota(i32, (chunk, deep), 1)

    def permute(c, carry):
        at = rows_at(c * chunk, chunk, chunk)
        want = jnp.concatenate([col_a[at, :]] * (deep // LANES), axis=1)
        total = jnp.zeros((chunk, LANES), f32)
        for k in range(rows // deep):
            pick = onehot(want - k * deep == lane)
            total = total + jnp.dot(pick, pay[pl.ds(k * deep, deep), :], preferred_element_type=f32)
        send[at, :] = total.astype(bf16)
        return carry

    lax.fori_loop(0, plan.chunks, permute, 0)
    pl.semaphore_wait(barrier, dev - 1)

    def send_tag(slot, carry):
        at = pl.ds(slot, 1)
        pltpu.make_async_remote_copy(
            src_ref=tag_send.at[at], dst_ref=tag_recv.at[at], send_sem=tag_sems.at[0], recv_sem=tag_sems.at[1],
            device_id=plan.partner(slot, 1), device_id_type=MESH_ID,
        ).start()
        return carry

    lax.fori_loop(1, dev, send_tag, 0)

    def send_row(slot, carry):
        at = rows_at(slot * SLOT, SLOT, SLOT)
        pltpu.make_async_remote_copy(
            src_ref=send.at[at], dst_ref=recv.at[at], send_sem=pay_send_sem,
            recv_sem=pay_sems.at[slot // plan.chunk_slots],
            device_id=plan.partner(slot, 1), device_id_type=MESH_ID,
        ).start()
        return carry

    lax.fori_loop(1, dev, send_row, 0)
    recv[pl.ds(0, SLOT), :] = send[pl.ds(0, SLOT), :]
    tag_recv[pl.ds(0, 1), :] = tag_send[pl.ds(0, 1), :]
    acc[...] = jnp.zeros_like(acc)
    back[...] = jnp.zeros_like(back)

    others = pl.ds(1, dev - 1)
    pltpu.make_async_copy(tag_send.at[others], tag_recv.at[others], tag_sems.at[1]).wait()
    for a in range(plan.row_lines):
        got = tag_recv[pl.ds(8 * a, 8), :]
        line_a[pl.ds(a, 1), :] = jnp.sum(jnp.where(mine, got, 0), axis=0, keepdims=True)
        line_b[pl.ds(a, 1), :] = pltpu.roll(jnp.sum(jnp.where(half, got, 0), axis=0, keepdims=True), LANES // 2, 1)
    column_form(line_a[...], col_a, plan)
    column_form(line_b[...], col_b, plan)
    keys = line_a[...]
    line_a[...] = jnp.where(keys < 0, -2, keys)

    def wait_chunk(c, src, dst, sem, first):
        at = rows_at(c * chunk, chunk, chunk) if not first else pl.ds(SLOT, chunk - SLOT)
        pltpu.make_async_copy(src.at[at], dst.at[at], sem).wait()

    def add_pairs(c):
        rhs = jnp.concatenate([recv[rows_at(c * chunk, chunk, chunk), :], jnp.ones((chunk, LANES), bf16)], axis=1)
        one, two = wide_line(line_a, c, plan), wide_line(line_b, c, plan)
        for b in range(rows // block):
            at = pl.ds(b * block, block)
            col_one = jnp.concatenate([col_a[at, :]] * (chunk // LANES), axis=1)
            col_two = jnp.concatenate([col_b[at, :]] * (chunk // LANES), axis=1)
            same = onehot((col_one == one) & (col_two == two))
            acc[at, :] += jnp.dot(same, rhs, preferred_element_type=f32)

    wait_chunk(0, send, recv, pay_sems.at[0], True)
    add_pairs(0)

    def pairs(c, carry):
        wait_chunk(c, send, recv, pay_sems.at[c], False)
        add_pairs(c)
        return carry

    lax.fori_loop(1, plan.chunks, pairs, 0)

    piece = min(256, rows)
    slots = piece // SLOT

    def send_back(slot, carry):
        at = rows_at(slot * SLOT, SLOT, SLOT)
        pltpu.make_async_remote_copy(
            src_ref=mean.at[at], dst_ref=ret.at[at], send_sem=ret_send_sem,
            recv_sem=ret_sems.at[slot // plan.chunk_slots],
            device_id=plan.partner(slot, -1), device_id_type=MESH_ID,
        ).start()
        return carry

    def finish(p, dups):
        at = rows_at(p * piece, piece, piece)
        count = acc[at, pl.ds(LANES, LANES)]
        inverse = 1.0 / jnp.maximum(count, 1.0)
        mean[at, :] = (acc[at, pl.ds(0, LANES)] * inverse).astype(bf16)
        again = jnp.where(count > 0.0, 1.0 - inverse, 0.0)
        return dups + jnp.sum(again.reshape(piece // 8, 8, LANES), axis=0)

    def finish_and_send(p, dups):
        dups = finish(p, dups)
        first = (p - 1) * slots
        lax.fori_loop(jnp.maximum(first, 1), first + slots, send_back, 0)
        return dups

    dups = finish(0, jnp.zeros((8, LANES), f32))
    dups = lax.fori_loop(1, rows // piece, finish_and_send, dups)
    dup_ref[...] = dups
    ret[pl.ds(0, SLOT), :] = mean[pl.ds(0, SLOT), :]
    lax.fori_loop(max(dev - slots, 1), dev, send_back, 0)

    def add_back(c, last):
        rhs = ret[rows_at(c * chunk, chunk, chunk), :]
        order = wide_line(ord_ref, c, plan)
        own = lax.broadcasted_iota(i32, (block, chunk), 0)
        for b in range(rows // block):
            at = pl.ds(b * block, block)
            pick = onehot(own == order - b * block)
            total = back[at, :] + jnp.dot(pick, rhs, preferred_element_type=f32)
            if last:
                pay[at, :] = total.astype(bf16)
            else:
                back[at, :] = total

    wait_chunk(0, mean, ret, ret_sems.at[0], True)
    add_back(0, False)

    def backs(c, carry):
        wait_chunk(c, mean, ret, ret_sems.at[c], False)
        add_back(c, False)
        return carry

    lax.fori_loop(1, plan.chunks - 1, backs, 0)
    wait_chunk(plan.chunks - 1, mean, ret, ret_sems.at[plan.chunks - 1], False)
    add_back(plan.chunks - 1, True)
    store = pltpu.make_async_copy(pay, out_hbm, io_sem)
    store.start()
    sent = pl.ds(SLOT, rows - SLOT)
    pltpu.make_async_copy(tag_send.at[others], tag_recv.at[others], tag_sems.at[0]).wait()
    pltpu.make_async_copy(send.at[sent], recv.at[sent], pay_send_sem).wait()
    pltpu.make_async_copy(mean.at[sent], ret.at[sent], ret_send_sem).wait()
    store.wait()


def exchange(plan, payload, order, key_one, key_two):
    rows, dev, lines = plan.rows, plan.devices, plan.row_lines
    vmem, hbm = pl.BlockSpec(memory_space=pltpu.VMEM), pl.BlockSpec(memory_space=pl.ANY)
    tile = lambda n, m, t: pltpu.VMEM((n, m), t)
    return pl.pallas_call(
        functools.partial(kernel, plan),
        out_shape=(jax.ShapeDtypeStruct((rows, LANES), bf16), jax.ShapeDtypeStruct((8, LANES), f32)),
        in_specs=[hbm, vmem, vmem, vmem],
        out_specs=(hbm, vmem),
        scratch_shapes=[
            *[tile(rows, LANES, bf16) for _ in range(5)],
            tile(rows, LANES, i32),
            tile(rows, LANES, i32),
            tile(dev, LANES, i32),
            tile(dev, LANES, i32),
            tile(lines, LANES, i32),
            tile(lines, LANES, i32),
            tile(rows, 2 * LANES, f32),
            tile(rows, LANES, f32),
            pltpu.SemaphoreType.DMA,
            pltpu.SemaphoreType.DMA((2,)),
            pltpu.SemaphoreType.DMA,
            pltpu.SemaphoreType.DMA((plan.chunks,)),
            pltpu.SemaphoreType.DMA,
            pltpu.SemaphoreType.DMA((plan.chunks,)),
        ],
        compiler_params=pltpu.CompilerParams(
            collective_id=0, has_side_effects=True, vmem_limit_bytes=48 * 2**20
        ),
        name="filter",
    )(payload, order, key_one, key_two)


def on_device(plan, payload, first_key, second_key, live, first_bucket, second_bucket):
    nz, nx, ny, nc = plan.dims
    coords = (first_bucket // nx, lax.rem(first_bucket, nx), second_bucket // nc, lax.rem(second_bucket, nc))
    place = plan.slot_of(coords) * plan.rows + lax.iota(i32, plan.rows)
    key_one = jnp.where(live > 0, first_key, -1)
    place, key_one, key_two = lax.sort((place, key_one, second_key), num_keys=1, is_stable=False)
    lines = (plan.row_lines, LANES)
    group_mean, dups = exchange(
        plan, payload, lax.rem(place, plan.rows).reshape(lines), key_one.reshape(lines), key_two.reshape(lines)
    )
    own = jnp.round(jnp.sum(dups[:, 0]))
    return group_mean, lax.psum(own, AXES).astype(i32)


def build(torus, plan):
    rows = P(AXES)
    return jax.shard_map(
        functools.partial(on_device, plan),
        mesh=torus,
        in_specs=(P(AXES, None), rows, rows, rows, rows, rows),
        out_specs=(P(AXES, None), P()),
        check_vma=False,
    )


def solution(mesh):
    dims = (8, 4, 4, 2)
    return build(Mesh(mesh.devices.reshape(dims), AXES), Plan(dims, 512, 1024))
```

```python
import functools

import jax
import jax.numpy as jnp
from jax import lax
from jax.experimental import pallas as pl
from jax.experimental.pallas import tpu as pltpu
from jax.sharding import Mesh
from jax.sharding import PartitionSpec as P

AXES = ("z", "x", "y", "c")
MESH_ID = pl.DeviceIdType.MESH
f32, bf16, i32 = jnp.float32, jnp.bfloat16, jnp.int32
SLOT = 16
LANES = 128


def onehot(mask):
    return jnp.where(mask, 1.0, 0.0).astype(bf16)


def rows_at(start, size, align):
    return pl.ds(pl.multiple_of(start, align), size)


class Plan:
    def __init__(self, dims, chunk, block, early, unrolled=False):
        self.dims = dims
        self.plane = dims[1] * dims[2] * dims[3]
        self.devices = dims[0] * self.plane
        self.units = dims[0]
        self.rows = self.devices * SLOT
        self.chunk = chunk
        self.chunks = self.rows // chunk
        self.chunk_slots = chunk // SLOT
        self.block = block
        self.early = early
        self.row_lines = self.rows // LANES
        self.unrolled = unrolled
        self.first = (dims[1] // 2, dims[2] // 2, dims[3] // 2)
        at = [(n - f) % n for n, f in zip(dims[1:], self.first)]
        self.own_rest = (at[0] * dims[2] + at[1]) * dims[3] + at[2]
        self.own_slot = self.devices - self.plane + self.own_rest

    def loop(self, low, high, body):
        if self.unrolled:
            for i in range(low, high):
                body(i)
        else:
            lax.fori_loop(low, high, lambda i, carry: (body(i), carry)[1], 0)

    def slot_of(self, coords):
        nz = self.dims[0]
        steps = [lax.rem(at - lax.axis_index(axis) + n, n) for n, axis, at in zip(self.dims, AXES, coords)]
        rest = jnp.zeros_like(steps[0])
        for n, f, step in zip(self.dims[1:], self.first, steps[1:]):
            rest = rest * n + lax.rem(step - f + n, n)
        far = jnp.minimum(steps[0], nz - steps[0])
        pair = self.plane + (nz // 2 - 1 - far) * 2 * self.plane + 2 * rest + (steps[0] > nz // 2).astype(i32)
        slot = jnp.where(far == nz // 2, rest, pair)
        return jnp.where(far == 0, self.devices - self.plane + rest, slot)


class Partners:
    def __init__(self, plan, sign):
        self.plan, self.sign = plan, sign
        self.me = [lax.axis_index(axis) for axis in AXES]
        nx, ny, nc = plan.dims[1:]
        self.tails = [
            (self.shift(2, ty + plan.first[1]), self.shift(3, tc + plan.first[2])) for ty in range(ny) for tc in range(nc)
        ]

    def shift(self, dim, step):
        n = self.plan.dims[dim]
        return lax.rem(self.me[dim] + (step if self.sign > 0 else 2 * n - step), n)

    def unit(self, u, act):
        plan = self.plan
        nz, nx = plan.dims[:2]
        width = len(self.tails)
        base = u * plan.plane
        if isinstance(u, int) and u == 0:
            ups = [(self.shift(0, nz // 2), 0)]
            low, high, origin, stride = 0, nx, 0, 1
        elif isinstance(u, int) and u == plan.units - 1:
            for tx in range(nx):
                for k, tail in enumerate(self.tails):
                    rest = tx * width + k
                    if rest != plan.own_rest:
                        act(base + rest, (self.me[0], self.shift(1, tx + plan.first[0]), *tail))
            return
        else:
            far = nz // 2 - 1 - (u - 1) // 2
            ups = [(self.shift(0, far), 0), (self.shift(0, nz - far), 1)]
            low, high, origin, stride = 0, nx // 2, lax.rem(u - 1, 2) * (nx // 2), 2

        def line(t, carry):
            x = self.shift(1, origin + t + plan.first[0])
            for k, tail in enumerate(self.tails):
                for z, plus in ups:
                    act(base + stride * (t * width + k) + plus, (z, x, *tail))
            return carry

        lax.fori_loop(low, high, line, 0)

    def all(self, act):
        self.unit(0, act)
        self.plan.loop(1, self.plan.units - 1, lambda u: self.unit(u, act))
        self.unit(self.plan.units - 1, act)


def column_form(lines, col_ref, plan):
    turned = jnp.transpose(lines)
    for b in range(plan.row_lines):
        col_ref[pl.ds(b * LANES, LANES), :] = jnp.broadcast_to(turned[:, b : b + 1], (LANES, LANES))


def wide_line(ref, chunk_index, plan):
    n = plan.chunk // LANES
    return jnp.concatenate([ref[pl.ds(chunk_index * n + t, 1), :] for t in range(n)], axis=1)


def kernel(plan, pay_hbm, ord_ref, k1_ref, k2_ref, out_ref, dup_ref, pay, send, recv, mean, ret, col_a, col_b,
           tag_send, tag_recv, line_a, line_b, acc, back, near, far, io_sem, tag_sems, pay_send_sem, pay_sems,
           ret_send_sem, ret_sems, dup_sems):
    dev, rows, chunk, block, plane = plan.devices, plan.rows, plan.chunk, plan.block, plan.plane
    to, source = Partners(plan, 1), Partners(plan, -1)
    load = pltpu.make_async_copy(pay_hbm, pay, io_sem)
    load.start()
    barrier = pltpu.get_barrier_semaphore()
    to.all(lambda slot, who: pl.semaphore_signal(barrier, inc=1, device_id=who, device_id_type=MESH_ID))

    part = lax.broadcasted_iota(i32, (8, LANES), 1) // SLOT
    sub = lax.broadcasted_iota(i32, (8, LANES), 0)
    mine = part == sub
    half = part == lax.rem(sub + 4, 8)
    for a in range(plan.row_lines):
        one = jnp.broadcast_to(k1_ref[pl.ds(a, 1), :], (8, LANES))
        two = jnp.broadcast_to(pltpu.roll(k2_ref[pl.ds(a, 1), :], LANES // 2, 1), (8, LANES))
        tag_send[pl.ds(8 * a, 8), :] = jnp.where(mine, one, two)
    column_form(ord_ref[...], col_a, plan)
    load.wait()

    deep = min(1024, rows)
    lane = lax.broadcasted_iota(i32, (chunk, deep), 1)

    def permute(c):
        at = rows_at(c * chunk, chunk, chunk)
        want = jnp.concatenate([col_a[at, :]] * (deep // LANES), axis=1)
        total = jnp.zeros((chunk, LANES), f32)
        for k in range(rows // deep):
            pick = onehot(want - k * deep == lane)
            total = total + jnp.dot(pick, pay[pl.ds(k * deep, deep), :], preferred_element_type=f32)
        send[at, :] = total.astype(bf16)

    def send_tag(slot, who):
        at = pl.ds(slot, 1)
        pltpu.make_async_remote_copy(
            src_ref=tag_send.at[at], dst_ref=tag_recv.at[at], send_sem=tag_sems.at[0], recv_sem=tag_sems.at[1],
            device_id=who, device_id_type=MESH_ID,
        ).start()

    def send_row(slot, who):
        at = rows_at(slot * SLOT, SLOT, SLOT)
        pltpu.make_async_remote_copy(
            src_ref=send.at[at], dst_ref=recv.at[at], send_sem=pay_send_sem,
            recv_sem=pay_sems.at[slot // plan.chunk_slots], device_id=who, device_id_type=MESH_ID,
        ).start()

    def send_chunk(group, c, act):
        per = plan.units // plan.chunks
        for i in range(per):
            group.unit(c * per + i, act)

    early = plan.early
    plan.loop(0, early, permute)
    pl.semaphore_wait(barrier, dev - 1)
    to.all(send_tag)
    send_chunk(to, 0, send_row)
    plan.loop(1, early - 1, lambda c: send_chunk(to, c, send_row))

    def permute_and_send(c):
        permute(c)
        send_chunk(to, c - 1, send_row)

    plan.loop(early, plan.chunks, permute_and_send)
    own = rows_at(plan.own_slot * SLOT, SLOT, SLOT)
    own_line = pl.ds(plan.own_slot, 1)
    recv[own, :] = send[own, :]
    tag_recv[own_line, :] = tag_send[own_line, :]
    acc[...] = jnp.zeros_like(acc)
    back[...] = jnp.zeros_like(back)
    send_chunk(to, plan.chunks - 1, send_row)

    others = pl.ds(0, dev - 1)
    pltpu.make_async_copy(tag_send.at[others], tag_recv.at[others], tag_sems.at[1]).wait()
    for a in range(plan.row_lines):
        got = tag_recv[pl.ds(8 * a, 8), :]
        line_a[pl.ds(a, 1), :] = jnp.sum(jnp.where(mine, got, 0), axis=0, keepdims=True)
        line_b[pl.ds(a, 1), :] = pltpu.roll(jnp.sum(jnp.where(half, got, 0), axis=0, keepdims=True), LANES // 2, 1)
    column_form(line_a[...], col_a, plan)
    column_form(line_b[...], col_b, plan)
    keys = line_a[...]
    line_a[...] = jnp.where(keys < 0, -2, keys)

    def wait_chunk(src, dst, sems, c, last=False):
        at = pl.ds(0, chunk - SLOT if last else chunk)
        pltpu.make_async_copy(src.at[at], dst.at[at], sems.at[c]).wait()

    def add_pairs(c):
        rhs = jnp.concatenate([recv[rows_at(c * chunk, chunk, chunk), :], jnp.ones((chunk, LANES), bf16)], axis=1)
        one, two = wide_line(line_a, c, plan), wide_line(line_b, c, plan)
        for b in range(rows // block):
            at = pl.ds(b * block, block)
            col_one = jnp.concatenate([col_a[at, :]] * (chunk // LANES), axis=1)
            col_two = jnp.concatenate([col_b[at, :]] * (chunk // LANES), axis=1)
            same = onehot((col_one == one) & (col_two == two))
            acc[at, :] += jnp.dot(same, rhs, preferred_element_type=f32)

    final = plan.chunks - 1

    def pairs(c):
        wait_chunk(send, recv, pay_sems, c)
        add_pairs(c)

    plan.loop(0, final, pairs)
    wait_chunk(send, recv, pay_sems, final, True)
    add_pairs(final)

    piece = min(256, chunk)

    def counts(p, dups):
        at = rows_at(p * piece, piece, piece)
        count = acc[at, pl.ds(LANES, LANES)]
        inverse = 1.0 / jnp.maximum(count, 1.0)
        acc[at, pl.ds(LANES, LANES)] = inverse
        again = jnp.where(count > 0.0, 1.0 - inverse, 0.0)
        return dups + jnp.sum(again.reshape(piece // 8, 8, LANES), axis=0)

    dups = lax.fori_loop(0, rows // piece, counts, jnp.zeros((8, LANES), f32))
    near[pl.ds(plan.own_rest, 1), :] = jnp.floor(jnp.sum(dups, axis=0, keepdims=True) + 0.5)

    def finish(p):
        at = rows_at(p * piece, piece, piece)
        mean[at, :] = (acc[at, pl.ds(0, LANES)] * acc[at, pl.ds(LANES, LANES)]).astype(bf16)

    def send_near(slot, who):
        rest = slot - (dev - plane)
        pltpu.make_async_remote_copy(
            src_ref=near.at[pl.ds(plan.own_rest, 1)], dst_ref=near.at[pl.ds(rest, 1)], send_sem=dup_sems.at[0],
            recv_sem=dup_sems.at[1], device_id=who, device_id_type=MESH_ID,
        ).start()

    def send_back(slot, who):
        at = rows_at(slot * SLOT, SLOT, SLOT)
        pltpu.make_async_remote_copy(
            src_ref=mean.at[at], dst_ref=ret.at[at], send_sem=ret_send_sem,
            recv_sem=ret_sems.at[slot // plan.chunk_slots], device_id=who, device_id_type=MESH_ID,
        ).start()

    pieces = chunk // piece

    def finish_chunk(c):
        for i in range(pieces):
            finish(c * pieces + i)

    def finish_and_send(c):
        finish_chunk(c)
        send_chunk(source, c - 1, send_back)

    finish_chunk(0)
    finish_chunk(1)
    to.unit(plan.units - 1, send_near)
    send_chunk(source, 0, send_back)
    plan.loop(2, plan.chunks, finish_and_send)
    ret[own, :] = mean[own, :]

    near_rows = pl.ds(0, plane - 1)
    pltpu.make_async_copy(near.at[near_rows], near.at[near_rows], dup_sems.at[1]).wait()
    far[pl.ds(0, 1), :] = jnp.sum(near[...], axis=0, keepdims=True)
    send_chunk(source, plan.chunks - 1, send_back)
    nz = plan.dims[0]
    for step in range(1, nz):
        pltpu.make_async_remote_copy(
            src_ref=far.at[pl.ds(0, 1)], dst_ref=far.at[pl.ds(step, 1)], send_sem=dup_sems.at[2],
            recv_sem=dup_sems.at[3], device_id=(to.shift(0, step), *to.me[1:]), device_id_type=MESH_ID,
        ).start()

    def add_back(c, last):
        rhs = ret[rows_at(c * chunk, chunk, chunk), :]
        order = wide_line(ord_ref, c, plan)
        own_row = lax.broadcasted_iota(i32, (block, chunk), 0)
        for b in range(rows // block):
            at = pl.ds(b * block, block)
            pick = onehot(own_row == order - b * block)
            total = back[at, :] + jnp.dot(pick, rhs, preferred_element_type=f32)
            if last:
                out_ref[at, :] = total.astype(bf16)
            else:
                back[at, :] = total

    def backs(c):
        wait_chunk(mean, ret, ret_sems, c)
        add_back(c, False)

    plan.loop(0, final, backs)
    far_rows = pl.ds(0, nz - 1)
    pltpu.make_async_copy(far.at[far_rows], far.at[far_rows], dup_sems.at[3]).wait()
    dup_ref[...] = jnp.broadcast_to(jnp.sum(far[...], axis=0, keepdims=True), (8, LANES))
    wait_chunk(mean, ret, ret_sems, final, True)
    add_back(final, True)
    sent = pl.ds(0, rows - SLOT)
    pltpu.make_async_copy(tag_send.at[others], tag_recv.at[others], tag_sems.at[0]).wait()
    pltpu.make_async_copy(send.at[sent], recv.at[sent], pay_send_sem).wait()
    pltpu.make_async_copy(mean.at[sent], ret.at[sent], ret_send_sem).wait()
    pltpu.make_async_copy(near.at[near_rows], near.at[near_rows], dup_sems.at[0]).wait()
    pltpu.make_async_copy(far.at[far_rows], far.at[far_rows], dup_sems.at[2]).wait()


def exchange(plan, payload, order, key_one, key_two):
    rows, dev, lines = plan.rows, plan.devices, plan.row_lines
    vmem, hbm = pl.BlockSpec(memory_space=pltpu.VMEM), pl.BlockSpec(memory_space=pltpu.HBM)
    tile = lambda n, m, t: pltpu.VMEM((n, m), t)
    return pl.pallas_call(
        functools.partial(kernel, plan),
        out_shape=(jax.ShapeDtypeStruct((rows, LANES), bf16), jax.ShapeDtypeStruct((8, LANES), f32)),
        in_specs=[hbm, vmem, vmem, vmem],
        out_specs=(vmem, vmem),
        scratch_shapes=[
            *[tile(rows, LANES, bf16) for _ in range(5)],
            tile(rows, LANES, i32),
            tile(rows, LANES, i32),
            tile(dev, LANES, i32),
            tile(dev, LANES, i32),
            tile(lines, LANES, i32),
            tile(lines, LANES, i32),
            tile(rows, 2 * LANES, f32),
            tile(rows, LANES, f32),
            tile(plan.plane, LANES, f32),
            tile(plan.dims[0], LANES, f32),
            pltpu.SemaphoreType.DMA,
            pltpu.SemaphoreType.DMA((2,)),
            pltpu.SemaphoreType.DMA,
            pltpu.SemaphoreType.DMA((plan.chunks,)),
            pltpu.SemaphoreType.DMA,
            pltpu.SemaphoreType.DMA((plan.chunks,)),
            pltpu.SemaphoreType.DMA((4,)),
        ],
        compiler_params=pltpu.CompilerParams(
            collective_id=0, has_side_effects=True, vmem_limit_bytes=48 * 2**20
        ),
        name="filter",
    )(payload, order, key_one, key_two)


def on_device(plan, payload, first_key, second_key, live, first_bucket, second_bucket):
    nz, nx, ny, nc = plan.dims
    coords = (first_bucket // nx, lax.rem(first_bucket, nx), second_bucket // nc, lax.rem(second_bucket, nc))
    place = plan.slot_of(coords) * plan.rows + lax.iota(i32, plan.rows)
    key_one = jnp.where(live > 0, first_key, -1)
    place, key_one, key_two = lax.sort((place, key_one, second_key), num_keys=1, is_stable=False)
    lines = (plan.row_lines, LANES)
    group_mean, dups = exchange(
        plan, payload, lax.rem(place, plan.rows).reshape(lines), key_one.reshape(lines), key_two.reshape(lines)
    )
    return group_mean, dups[0, 0].astype(i32)


def build(torus, plan):
    rows = P(AXES)
    return jax.shard_map(
        functools.partial(on_device, plan),
        mesh=torus,
        in_specs=(P(AXES, None), rows, rows, rows, rows, rows),
        out_specs=(P(AXES, None), P()),
        check_vma=False,
    )


def solution(mesh):
    dims = (8, 4, 4, 2)
    return build(Mesh(mesh.devices.reshape(dims), AXES), Plan(dims, 512, 1024, 4))
```

```python
import functools

import jax
import jax.numpy as jnp
from jax import lax
from jax.experimental import pallas as pl
from jax.experimental.pallas import tpu as pltpu
from jax.sharding import Mesh
from jax.sharding import PartitionSpec as P

AXES = ("z", "x", "y", "c")
MESH_ID = pl.DeviceIdType.MESH
f32, bf16, i32 = jnp.float32, jnp.bfloat16, jnp.int32
SLOT = 16
LANES = 128


def onehot(mask):
    return jnp.where(mask, 1.0, 0.0).astype(bf16)


def rows_at(start, size, align):
    return pl.ds(pl.multiple_of(start, align), size)


class Plan:
    def __init__(self, dims, block, unrolled=False):
        nz, nx, ny, nc = self.dims = dims
        self.unit = nz * nx
        self.units = ny * nc
        self.devices = self.unit * self.units
        self.rows = self.devices * SLOT
        self.chunk = self.unit * SLOT
        self.block = block
        self.row_lines = self.rows // LANES
        self.unrolled = unrolled
        self.z_steps = [nz // 2]
        for far in range(nz // 2 - 1, 0, -1):
            self.z_steps += [far, nz - far]
        self.z_steps.append(0)

    def loop(self, low, high, body):
        if self.unrolled:
            for i in range(low, high):
                body(i)
        else:
            lax.fori_loop(low, high, lambda i, carry: (body(i), carry)[1], 0)

    def slot_of(self, first_bucket, second_bucket):
        nz, nx, ny, nc = self.dims
        coords = (
            lax.shift_right_logical(first_bucket, nx.bit_length() - 1), first_bucket & (nx - 1),
            lax.shift_right_logical(second_bucket, nc.bit_length() - 1), second_bucket & (nc - 1),
        )
        z, x, y, c = [(at - lax.axis_index(axis)) & (n - 1) for n, axis, at in zip(self.dims, AXES, coords)]
        far = jnp.minimum(z, nz - z)
        z_at = (nz // 2 - 1 - far) * 2 + 1 + jnp.where(z > nz // 2, 1, 0)
        z_at = jnp.where(far == nz // 2, 0, z_at)
        turn = ((y - x) & (ny - 1)) * nc + c
        return (self.units - 1 - turn) * self.unit + z_at * nx + nx - 1 - x


class Partners:
    def __init__(self, plan, sign):
        self.plan, self.sign = plan, sign
        self.me = [lax.axis_index(axis) for axis in AXES]
        self.z = [self.shift(0, step) for step in plan.z_steps]
        self.x = [self.shift(1, step) for step in range(plan.dims[1] - 1, -1, -1)]

    def shift(self, dim, step):
        n = self.plan.dims[dim]
        return lax.rem(self.me[dim] + (step if self.sign > 0 else 2 * n - step), n)

    def each(self, u, act):
        plan = self.plan
        nz, nx, ny, nc = plan.dims
        turn = plan.units - 1 - u
        c = self.shift(3, turn % nc if isinstance(u, int) else lax.rem(turn, nc))
        y_turn = turn // nc if isinstance(u, int) else lax.div(turn, nc)
        y = [self.shift(2, (y_turn + step) % ny if isinstance(u, int) else lax.rem(y_turn + step, ny)) for step in range(nx - 1, -1, -1)]
        for i, z in enumerate(self.z):
            for k, x in enumerate(self.x):
                if isinstance(u, int) and u == plan.units - 1 and i == nz - 1 and k == nx - 1:
                    continue
                act(u * plan.unit + i * nx + k, (z, x, y[k], c))

    def greet(self, barrier):
        plan = self.plan
        nz, nx, ny, nc = plan.dims
        tails = [(self.shift(2, y + ny // 2), self.shift(3, c + 1)) for y in range(ny) for c in range(nc)]
        for i, z in enumerate(self.z):
            for k in range(nx):
                for j, tail in enumerate(tails):
                    own = i == nz - 1 and (k + nx // 2) % nx == 0 and (j // nc + ny // 2) % ny == 0 and (j + 1) % nc == 0
                    if not own:
                        who = (z, self.x[(nx // 2 - 1 - k) % nx], *tail)
                        pl.semaphore_signal(barrier, inc=1, device_id=who, device_id_type=MESH_ID)


def sorted_lines(key, others):
    lines = key.shape[0]
    row, lane = lax.broadcasted_iota(i32, key.shape, 0), lax.broadcasted_iota(i32, key.shape, 1)

    def bit(size):
        at, size = (lane, size) if size < LANES else (row, size // LANES)
        return lax.shift_right_logical(at, size.bit_length() - 1) & 1

    size = 2
    while size <= lines * LANES:
        step = size // 2
        while step:
            upper = bit(step)
            keep_max = upper != bit(size) if size < lines * LANES else upper == 1
            axis, by, span = (1, step, LANES) if step < LANES else (0, step // LANES, lines)

            def other(a, upper=upper, axis=axis, by=by, span=span):
                return jnp.where(upper == 1, pltpu.roll(a, by, axis), pltpu.roll(a, span - by, axis))

            there = other(key)
            new = jnp.where(keep_max, jnp.maximum(key, there), jnp.minimum(key, there))
            moved = new != key
            others = [jnp.where(moved, other(a), a) for a in others]
            key = new
            step //= 2
        size *= 2
    return key, others


def column_form(lines, col_ref, plan):
    turned = jnp.transpose(lines)
    for b in range(plan.row_lines):
        col_ref[pl.ds(b * LANES, LANES), :] = jnp.broadcast_to(turned[:, b : b + 1], (LANES, LANES))


def wide_line(ref, chunk_index, plan):
    n = plan.chunk // LANES
    return jnp.concatenate([ref[pl.ds(chunk_index * n + t, 1), :] for t in range(n)], axis=1)


def kernel(plan, pay_hbm, *refs):
    body(plan, pay_hbm, refs[:3], *refs[3:])


def body(plan, pay_hbm, small, out_ref, dup_ref, fields, ord_ref, pay, send, recv, mean, ret, col_a, col_b,
           tag_send, tag_recv, line_a, line_b, acc, back, near, far, io_sem, tag_sems, pay_send_sem, pay_sems,
           ret_send_sem, ret_sems, dup_sems, field_sems):
    dev, rows, chunk, block = plan.devices, plan.rows, plan.chunk, plan.block
    last_unit = plan.units - 1
    to, source = Partners(plan, 1), Partners(plan, -1)
    loads = [pltpu.make_async_copy(ref, fields.at[i], field_sems.at[i]) for i, ref in enumerate(small)]
    load = pltpu.make_async_copy(pay_hbm, pay, io_sem)
    for each in (*loads, load):
        each.start()
    barrier = pltpu.get_barrier_semaphore()
    to.greet(barrier)

    for each in loads:
        each.wait()
    place, (first_key, second_key) = sorted_lines(fields[0], [fields[1], fields[2]])
    order = place & (rows - 1)
    ord_ref[...] = order
    second_key = pltpu.roll(second_key, LANES // 2, 1)

    part = lax.broadcasted_iota(i32, (8, LANES), 1) // SLOT
    sub = lax.broadcasted_iota(i32, (8, LANES), 0)
    mine = part == sub
    half = part == lax.rem(sub + 4, 8)
    for a in range(plan.row_lines):
        one = jnp.broadcast_to(first_key[a : a + 1, :], (8, LANES))
        two = jnp.broadcast_to(second_key[a : a + 1, :], (8, LANES))
        tag_send[pl.ds(8 * a, 8), :] = jnp.where(mine, one, two)
    column_form(order, col_a, plan)
    load.wait()

    deep = min(1024, rows)
    lane = lax.broadcasted_iota(i32, (chunk, deep), 1)

    def permute(c):
        at = rows_at(c * chunk, chunk, chunk)
        want = jnp.concatenate([col_a[at, :]] * (deep // LANES), axis=1)
        total = jnp.zeros((chunk, LANES), f32)
        for k in range(rows // deep):
            pick = onehot(want - k * deep == lane)
            total = total + jnp.dot(pick, pay[pl.ds(k * deep, deep), :], preferred_element_type=f32)
        send[at, :] = total.astype(bf16)

    def send_tag(slot, who):
        at = pl.ds(slot, 1)
        pltpu.make_async_remote_copy(
            src_ref=tag_send.at[at], dst_ref=tag_recv.at[at], send_sem=tag_sems.at[0], recv_sem=tag_sems.at[1],
            device_id=who, device_id_type=MESH_ID,
        ).start()

    def send_row(slot, who):
        at = rows_at(slot * SLOT, SLOT, SLOT)
        pltpu.make_async_remote_copy(
            src_ref=send.at[at], dst_ref=recv.at[at], send_sem=pay_send_sem,
            recv_sem=pay_sems.at[slot // plan.unit], device_id=who, device_id_type=MESH_ID,
        ).start()

    pl.semaphore_wait(barrier, dev - 1)
    plan.loop(0, plan.units // 2, lambda u: to.each(u, send_tag))
    permute(0)
    plan.loop(plan.units // 2, last_unit, lambda u: to.each(u, send_tag))
    to.each(last_unit, send_tag)
    to.each(0, send_row)
    permute(1)

    def permute_and_send(u):
        permute(u)
        to.each(u - 1, send_row)

    plan.loop(2, plan.units, permute_and_send)
    own = pl.ds(rows - SLOT, SLOT)
    own_line = pl.ds(dev - 1, 1)
    recv[own, :] = send[own, :]
    tag_recv[own_line, :] = tag_send[own_line, :]
    acc[...] = jnp.zeros_like(acc)
    back[...] = jnp.zeros_like(back)
    to.each(last_unit, send_row)

    others = pl.ds(0, dev - 1)
    pltpu.make_async_copy(tag_send.at[others], tag_recv.at[others], tag_sems.at[1]).wait()
    for a in range(plan.row_lines):
        got = tag_recv[pl.ds(8 * a, 8), :]
        line_a[pl.ds(a, 1), :] = jnp.sum(jnp.where(mine, got, 0), axis=0, keepdims=True)
        line_b[pl.ds(a, 1), :] = pltpu.roll(jnp.sum(jnp.where(half, got, 0), axis=0, keepdims=True), LANES // 2, 1)
    column_form(line_a[...], col_a, plan)
    column_form(line_b[...], col_b, plan)
    keys = line_a[...]
    line_a[...] = jnp.where(keys < 0, -2, keys)

    def wait_chunk(src, dst, sems, c, last=False):
        at = pl.ds(0, chunk - SLOT if last else chunk)
        pltpu.make_async_copy(src.at[at], dst.at[at], sems.at[c]).wait()

    def add_pairs(c):
        rhs = jnp.concatenate([recv[rows_at(c * chunk, chunk, chunk), :], jnp.ones((chunk, LANES), bf16)], axis=1)
        one, two = wide_line(line_a, c, plan), wide_line(line_b, c, plan)
        for b in range(rows // block):
            at = pl.ds(b * block, block)
            col_one = jnp.concatenate([col_a[at, :]] * (chunk // LANES), axis=1)
            col_two = jnp.concatenate([col_b[at, :]] * (chunk // LANES), axis=1)
            same = onehot((col_one == one) & (col_two == two))
            acc[at, :] += jnp.dot(same, rhs, preferred_element_type=f32)

    final = last_unit

    def pairs(c):
        wait_chunk(send, recv, pay_sems, c)
        add_pairs(c)

    plan.loop(0, final, pairs)
    wait_chunk(send, recv, pay_sems, final, True)
    add_pairs(final)

    piece = min(256, chunk)
    nz, nx, ny, nc = plan.dims
    plane = nx * ny * nc
    own_near = pl.ds(plane - 1, 1)

    def counts(p, dups):
        at = rows_at(p * piece, piece, piece)
        count = acc[at, pl.ds(LANES, LANES)]
        inverse = 1.0 / jnp.maximum(count, 1.0)
        acc[at, pl.ds(LANES, LANES)] = inverse
        again = jnp.where(count > 0.0, 1.0 - inverse, 0.0)
        return dups + jnp.sum(again.reshape(piece // 8, 8, LANES), axis=0)

    dups = lax.fori_loop(0, rows // piece, counts, jnp.zeros((8, LANES), f32))
    near[own_near, :] = jnp.floor(jnp.sum(dups, axis=0, keepdims=True) + 0.5)

    def finish(p):
        at = rows_at(p * piece, piece, piece)
        mean[at, :] = (acc[at, pl.ds(0, LANES)] * acc[at, pl.ds(LANES, LANES)]).astype(bf16)

    def send_near(step, who):
        pltpu.make_async_remote_copy(
            src_ref=near.at[own_near], dst_ref=near.at[pl.ds(step, 1)], send_sem=dup_sems.at[0],
            recv_sem=dup_sems.at[1], device_id=who, device_id_type=MESH_ID,
        ).start()

    def send_back(slot, who):
        at = rows_at(slot * SLOT, SLOT, SLOT)
        pltpu.make_async_remote_copy(
            src_ref=mean.at[at], dst_ref=ret.at[at], send_sem=ret_send_sem,
            recv_sem=ret_sems.at[slot // plan.unit], device_id=who, device_id_type=MESH_ID,
        ).start()

    pieces = chunk // piece

    def finish_chunk(c):
        for i in range(pieces):
            finish(c * pieces + i)

    def finish_and_send(u):
        finish_chunk(u)
        source.each(u - 1, send_back)

    finish_chunk(0)
    finish_chunk(1)
    for step in range(plane - 1, 0, -1):
        send_near(
            plane - 1 - step, (to.me[0], to.shift(1, step // (ny * nc)), to.shift(2, step // nc % ny), to.shift(3, step % nc))
        )
    source.each(0, send_back)
    plan.loop(2, plan.units, finish_and_send)
    ret[own, :] = mean[own, :]

    near_rows = pl.ds(0, plane - 1)
    pltpu.make_async_copy(near.at[near_rows], near.at[near_rows], dup_sems.at[1]).wait()
    far[pl.ds(0, 1), :] = jnp.sum(near[...], axis=0, keepdims=True)
    source.each(last_unit, send_back)
    for step in range(1, nz):
        pltpu.make_async_remote_copy(
            src_ref=far.at[pl.ds(0, 1)], dst_ref=far.at[pl.ds(step, 1)], send_sem=dup_sems.at[2],
            recv_sem=dup_sems.at[3], device_id=(to.shift(0, step), *to.me[1:]), device_id_type=MESH_ID,
        ).start()

    def add_back(c, last):
        rhs = ret[rows_at(c * chunk, chunk, chunk), :]
        order = wide_line(ord_ref, c, plan)
        own_row = lax.broadcasted_iota(i32, (block, chunk), 0)
        for b in range(rows // block):
            at = pl.ds(b * block, block)
            pick = onehot(own_row == order - b * block)
            total = back[at, :] + jnp.dot(pick, rhs, preferred_element_type=f32)
            if last:
                out_ref[at, :] = total.astype(bf16)
            else:
                back[at, :] = total

    def backs(c):
        wait_chunk(mean, ret, ret_sems, c)
        add_back(c, False)

    plan.loop(0, final, backs)
    far_rows = pl.ds(0, nz - 1)
    pltpu.make_async_copy(far.at[far_rows], far.at[far_rows], dup_sems.at[3]).wait()
    dup_ref[...] = jnp.broadcast_to(jnp.sum(far[...], axis=0, keepdims=True), (8, LANES)).astype(i32)
    wait_chunk(mean, ret, ret_sems, final, True)
    add_back(final, True)
    sent = pl.ds(0, rows - SLOT)
    pltpu.make_async_copy(tag_send.at[others], tag_recv.at[others], tag_sems.at[0]).wait()
    pltpu.make_async_copy(send.at[sent], recv.at[sent], pay_send_sem).wait()
    pltpu.make_async_copy(mean.at[sent], ret.at[sent], ret_send_sem).wait()
    pltpu.make_async_copy(near.at[near_rows], near.at[near_rows], dup_sems.at[0]).wait()
    pltpu.make_async_copy(far.at[far_rows], far.at[far_rows], dup_sems.at[2]).wait()


def on_device(plan, payload, first_key, second_key, live, first_bucket, second_bucket):
    rows, dev, lines = plan.rows, plan.devices, plan.row_lines
    hbm = pl.BlockSpec(memory_space=pltpu.HBM)
    place = plan.slot_of(first_bucket, second_bucket) * rows + lax.iota(i32, rows)
    columns = (place, jnp.where(live > 0, first_key, -1), second_key)
    tile = lambda n, m, t: pltpu.VMEM((n, m), t)
    group_mean, dups = pl.pallas_call(
        functools.partial(kernel, plan),
        out_shape=(jax.ShapeDtypeStruct((rows, LANES), bf16), jax.ShapeDtypeStruct((8, LANES), i32)),
        in_specs=[hbm] * 4,
        out_specs=(pl.BlockSpec(memory_space=pltpu.VMEM),) * 2,
        scratch_shapes=[
            pltpu.VMEM((3, lines, LANES), i32),
            tile(lines, LANES, i32),
            *[tile(rows, LANES, bf16) for _ in range(5)],
            tile(rows, LANES, i32),
            tile(rows, LANES, i32),
            tile(dev, LANES, i32),
            tile(dev, LANES, i32),
            tile(lines, LANES, i32),
            tile(lines, LANES, i32),
            tile(rows, 2 * LANES, f32),
            tile(rows, LANES, f32),
            tile(plan.devices // plan.dims[0], LANES, f32),
            tile(plan.dims[0], LANES, f32),
            pltpu.SemaphoreType.DMA,
            pltpu.SemaphoreType.DMA((2,)),
            pltpu.SemaphoreType.DMA,
            pltpu.SemaphoreType.DMA((plan.units,)),
            pltpu.SemaphoreType.DMA,
            pltpu.SemaphoreType.DMA((plan.units,)),
            pltpu.SemaphoreType.DMA((4,)),
            pltpu.SemaphoreType.DMA((3,)),
        ],
        compiler_params=pltpu.CompilerParams(
            collective_id=0, has_side_effects=True, vmem_limit_bytes=52 * 2**20
        ),
        name="filter",
    )(payload, *[column.reshape(lines, LANES) for column in columns])
    return group_mean, dups[0, 0]


def build(torus, plan):
    rows = P(AXES)
    return jax.shard_map(
        functools.partial(on_device, plan),
        mesh=torus,
        in_specs=(P(AXES, None), rows, rows, rows, rows, rows),
        out_specs=(P(AXES, None), P()),
        check_vma=False,
    )


def solution(mesh):
    dims = (8, 4, 4, 2)
    return build(Mesh(mesh.devices.reshape(dims), AXES), Plan(dims, 1024))
```

```python
import functools

import jax
import jax.numpy as jnp
from jax import lax
from jax.experimental import pallas as pl
from jax.experimental.pallas import tpu as pltpu
from jax.sharding import Mesh
from jax.sharding import PartitionSpec as P

AXES = ("z", "x", "y", "c")
MESH_ID = pl.DeviceIdType.MESH
f32, bf16, i32 = jnp.float32, jnp.bfloat16, jnp.int32
SLOT = 16
LANES = 128


def onehot(mask):
    return jnp.where(mask, 1.0, 0.0).astype(bf16)


def when(condition, act):
    if not isinstance(condition, bool):
        pl.when(condition)(act)
    elif condition:
        act()


def rows_at(start, size, align):
    return pl.ds(pl.multiple_of(start, align), size)


class Plan:
    def __init__(self, dims, block, unrolled=False):
        nz, nx, ny, nc = self.dims = dims
        self.unit = nz * nx
        self.units = ny * nc
        self.devices = self.unit * self.units
        self.rows = self.devices * SLOT
        self.chunk = self.unit * SLOT
        self.block = block
        self.row_lines = self.rows // LANES
        self.unrolled = unrolled
        self.z_steps = [nz // 2]
        for far in range(nz // 2 - 1, 0, -1):
            self.z_steps += [far, nz - far]
        self.z_steps.append(0)

    def loop(self, low, high, body):
        if self.unrolled:
            for i in range(low, high):
                body(i)
        else:
            lax.fori_loop(low, high, lambda i, carry: (body(i), carry)[1], 0)

    def slot_of(self, first_bucket, second_bucket):
        nz, nx, ny, nc = self.dims
        coords = (
            lax.shift_right_logical(first_bucket, nx.bit_length() - 1), first_bucket & (nx - 1),
            lax.shift_right_logical(second_bucket, nc.bit_length() - 1), second_bucket & (nc - 1),
        )
        z, x, y, c = [(at - lax.axis_index(axis)) & (n - 1) for n, axis, at in zip(self.dims, AXES, coords)]
        far = jnp.minimum(z, nz - z)
        z_at = (nz // 2 - 1 - far) * 2 + 1 + jnp.where(z > nz // 2, 1, 0)
        z_at = jnp.where(far == nz // 2, 0, z_at)
        turn = ((y - x) & (ny - 1)) * nc + c
        return (self.units - 1 - turn) * self.unit + z_at * nx + nx - 1 - x


class Partners:
    def __init__(self, plan, sign):
        self.plan, self.sign = plan, sign
        self.me = [lax.axis_index(axis) for axis in AXES]
        self.z = [self.shift(0, step) for step in plan.z_steps]
        self.x = [self.shift(1, step) for step in range(plan.dims[1] - 1, -1, -1)]

    def shift(self, dim, step):
        n = self.plan.dims[dim]
        return lax.rem(self.me[dim] + (step if self.sign > 0 else 2 * n - step), n)

    def each(self, u, act):
        plan = self.plan
        nz, nx, ny, nc = plan.dims
        turn = plan.units - 1 - u
        c = self.shift(3, turn % nc if isinstance(u, int) else lax.rem(turn, nc))
        y_turn = turn // nc if isinstance(u, int) else lax.div(turn, nc)
        y = [self.shift(2, (y_turn + step) % ny if isinstance(u, int) else lax.rem(y_turn + step, ny)) for step in range(nx - 1, -1, -1)]
        for i, z in enumerate(self.z):
            for k, x in enumerate(self.x):
                if isinstance(u, int) and u == plan.units - 1 and i == nz - 1 and k == nx - 1:
                    continue
                act(u * plan.unit + i * nx + k, (z, x, y[k], c))

    def greet(self, barrier):
        plan = self.plan
        nz, nx, ny, nc = plan.dims
        tails = [(self.shift(2, y + ny // 2), self.shift(3, c + 1)) for y in range(ny) for c in range(nc)]
        for i, z in enumerate(self.z):
            for k in range(nx):
                for j, tail in enumerate(tails):
                    own = i == nz - 1 and (k + nx // 2) % nx == 0 and (j // nc + ny // 2) % ny == 0 and (j + 1) % nc == 0
                    if not own:
                        who = (z, self.x[(nx // 2 - 1 - k) % nx], *tail)
                        pl.semaphore_signal(barrier, inc=1, device_id=who, device_id_type=MESH_ID)


def sorted_lines(key, others):
    lines = key.shape[0]
    row, lane = lax.broadcasted_iota(i32, key.shape, 0), lax.broadcasted_iota(i32, key.shape, 1)

    def bit(size):
        at, size = (lane, size) if size < LANES else (row, size // LANES)
        return lax.shift_right_logical(at, size.bit_length() - 1) & 1

    size = 2
    while size <= lines * LANES:
        step = size // 2
        while step:
            upper = bit(step)
            keep_max = upper != bit(size) if size < lines * LANES else upper == 1
            axis, by, span = (1, step, LANES) if step < LANES else (0, step // LANES, lines)

            def other(a, upper=upper, axis=axis, by=by, span=span):
                return jnp.where(upper == 1, pltpu.roll(a, by, axis), pltpu.roll(a, span - by, axis))

            there = other(key)
            new = jnp.where(keep_max, jnp.maximum(key, there), jnp.minimum(key, there))
            moved = new != key
            others = [jnp.where(moved, other(a), a) for a in others]
            key = new
            step //= 2
        size *= 2
    return key, others


def column_form(lines, col_ref, plan):
    turned = jnp.transpose(lines)
    for b in range(plan.row_lines):
        col_ref[pl.ds(b * LANES, LANES), :] = jnp.broadcast_to(turned[:, b : b + 1], (LANES, LANES))


def wide_line(ref, chunk_index, plan):
    n = plan.chunk // LANES
    return jnp.concatenate([ref[pl.ds(chunk_index * n + t, 1), :] for t in range(n)], axis=1)


def kernel(plan, pay_hbm, *refs):
    body(plan, pay_hbm, refs[:3], *refs[3:])


def body(plan, pay_hbm, small, out_ref, dup_ref, fields, ord_ref, pay, send, recv, mean, ret, col_a, col_b,
           tag_send, tag_recv, tag_other, line_a, line_b, acc, back, near, far, io_sem, tag_sems, pay_send_sem, pay_sems,
           ret_send_sem, ret_sems, dup_sems, field_sems):
    dev, rows, chunk, block = plan.devices, plan.rows, plan.chunk, plan.block
    last_unit = plan.units - 1
    to, source = Partners(plan, 1), Partners(plan, -1)
    loads = [pltpu.make_async_copy(ref, fields.at[i], field_sems.at[i]) for i, ref in enumerate(small)]
    load = pltpu.make_async_copy(pay_hbm, pay, io_sem)
    for each in (*loads, load):
        each.start()
    barrier = pltpu.get_barrier_semaphore()
    to.greet(barrier)

    for each in loads:
        each.wait()
    place, (first_key, second_key) = sorted_lines(fields[0], [fields[1], fields[2]])
    order = place & (rows - 1)
    ord_ref[...] = order
    second_key = pltpu.roll(second_key, LANES // 2, 1)

    part = lax.broadcasted_iota(i32, (8, LANES), 1) // SLOT
    sub = lax.broadcasted_iota(i32, (8, LANES), 0)
    spots = [part == lax.rem(sub + q, 8) for q in (0, 4, 2, 6)]
    quarter = LANES // 4
    tagged = [first_key, second_key, pltpu.roll(first_key, quarter, 1), pltpu.roll(second_key, quarter, 1)]
    unit_lines = plan.unit // 8
    pairs_of_units = plan.units // 2
    for v in range(pairs_of_units):
        for i in range(unit_lines):
            other, like = 2 * v * unit_lines + i, (2 * v + 1) * unit_lines + i
            one, two, three, four = [
                jnp.broadcast_to(keys[at : at + 1, :], (8, LANES)) for keys, at in zip(tagged, (like, like, other, other))
            ]
            line = jnp.where(spots[0], one, jnp.where(spots[1], two, jnp.where(spots[2], three, four)))
            tag_send[pl.ds(v * plan.unit + 8 * i, 8), :] = line
    column_form(order, col_a, plan)
    load.wait()

    deep = min(1024, rows)
    lane = lax.broadcasted_iota(i32, (chunk, deep), 1)

    def permute(c):
        at = rows_at(c * chunk, chunk, chunk)
        want = jnp.concatenate([col_a[at, :]] * (deep // LANES), axis=1)
        total = jnp.zeros((chunk, LANES), f32)
        for k in range(rows // deep):
            pick = onehot(want - k * deep == lane)
            total = total + jnp.dot(pick, pay[pl.ds(k * deep, deep), :], preferred_element_type=f32)
        send[at, :] = total.astype(bf16)

    def send_tags(v):
        def send_tag(slot, who):
            at = pl.ds(slot - plan.unit * (v + 1), 1)
            pltpu.make_async_remote_copy(
                src_ref=tag_send.at[at], dst_ref=tag_recv.at[at], send_sem=tag_sems.at[0], recv_sem=tag_sems.at[1],
                device_id=who, device_id_type=MESH_ID,
            ).start()

        to.each(2 * v + 1, send_tag)

    def send_row(slot, who):
        at = rows_at(slot * SLOT, SLOT, SLOT)
        pltpu.make_async_remote_copy(
            src_ref=send.at[at], dst_ref=recv.at[at], send_sem=pay_send_sem,
            recv_sem=pay_sems.at[slot // plan.unit], device_id=who, device_id_type=MESH_ID,
        ).start()

    pl.semaphore_wait(barrier, dev - 1)
    plan.loop(0, pairs_of_units // 2, send_tags)

    def first_sent():
        plan.loop(pairs_of_units // 2, pairs_of_units - 1, send_tags)
        send_tags(pairs_of_units - 1)
        to.each(0, send_row)

    def permute_and_send(u):
        permute(u)
        when(u == 0, first_sent)
        when(u >= 2, lambda: to.each(u - 1, send_row))

    plan.loop(0, plan.units, permute_and_send)
    lines = dev // 2
    others, own_line = pl.ds(0, lines - 1), pl.ds(lines - 1, 1)
    tag_recv[own_line, :] = tag_send[own_line, :]
    own = pl.ds(rows - SLOT, SLOT)
    recv[own, :] = send[own, :]
    pltpu.make_async_copy(tag_send.at[others], tag_recv.at[others], tag_sems.at[1]).wait()
    forward = pltpu.make_async_remote_copy(
        src_ref=tag_recv, dst_ref=tag_other, send_sem=tag_sems.at[2], recv_sem=tag_sems.at[3],
        device_id=(*to.me[:3], to.shift(3, 1)), device_id_type=MESH_ID,
    )
    to.each(last_unit, send_row)
    forward.start()
    acc[...] = jnp.zeros_like(acc)
    back[...] = jnp.zeros_like(back)

    def take(ref, v, i, line, at, by):
        got = ref[pl.ds(v * plan.unit + 8 * i, 8), :]
        one, two = [jnp.sum(jnp.where(spot, got, 0), axis=0, keepdims=True) for spot in spots[at : at + 2]]
        line_a[pl.ds(line, 1), :] = pltpu.roll(one, by, 1) if by else one
        line_b[pl.ds(line, 1), :] = pltpu.roll(two, (LANES // 2 + by) % LANES, 1)

    for v in range(pairs_of_units):
        for i in range(unit_lines):
            take(tag_recv, v, i, (2 * v + 1) * unit_lines + i, 0, 0)
    forward.wait_recv()
    for v in range(pairs_of_units):
        for i in range(unit_lines):
            take(tag_other, v, i, 2 * v * unit_lines + i, 2, LANES - quarter)
    column_form(line_a[...], col_a, plan)
    column_form(line_b[...], col_b, plan)
    keys = line_a[...]
    line_a[...] = jnp.where(keys < 0, -2, keys)

    def wait_chunk(src, dst, sems, c, last=False):
        at = pl.ds(0, chunk - SLOT if last else chunk)
        pltpu.make_async_copy(src.at[at], dst.at[at], sems.at[c]).wait()

    def add_pairs(c):
        rhs = jnp.concatenate([recv[rows_at(c * chunk, chunk, chunk), :], jnp.ones((chunk, LANES), bf16)], axis=1)
        one, two = wide_line(line_a, c, plan), wide_line(line_b, c, plan)
        for b in range(rows // block):
            at = pl.ds(b * block, block)
            col_one = jnp.concatenate([col_a[at, :]] * (chunk // LANES), axis=1)
            col_two = jnp.concatenate([col_b[at, :]] * (chunk // LANES), axis=1)
            same = onehot((col_one == one) & (col_two == two))
            acc[at, :] += jnp.dot(same, rhs, preferred_element_type=f32)

    final = last_unit

    def pairs(c):
        wait_chunk(send, recv, pay_sems, c)
        add_pairs(c)

    plan.loop(0, final, pairs)
    wait_chunk(send, recv, pay_sems, final, True)
    add_pairs(final)

    piece = min(256, chunk)
    nz, nx, ny, nc = plan.dims
    plane = nx * ny * nc
    own_near = pl.ds(plane - 1, 1)

    def counts(p, dups):
        at = rows_at(p * piece, piece, piece)
        count = acc[at, pl.ds(LANES, LANES)]
        inverse = 1.0 / jnp.maximum(count, 1.0)
        acc[at, pl.ds(LANES, LANES)] = inverse
        again = jnp.where(count > 0.0, 1.0 - inverse, 0.0)
        return dups + jnp.sum(again.reshape(piece // 8, 8, LANES), axis=0)

    dups = lax.fori_loop(0, rows // piece, counts, jnp.zeros((8, LANES), f32))
    near[own_near, :] = jnp.floor(jnp.sum(dups, axis=0, keepdims=True) + 0.5)

    def finish(p):
        at = rows_at(p * piece, piece, piece)
        mean[at, :] = (acc[at, pl.ds(0, LANES)] * acc[at, pl.ds(LANES, LANES)]).astype(bf16)

    def send_near(step, who):
        pltpu.make_async_remote_copy(
            src_ref=near.at[own_near], dst_ref=near.at[pl.ds(step, 1)], send_sem=dup_sems.at[0],
            recv_sem=dup_sems.at[1], device_id=who, device_id_type=MESH_ID,
        ).start()

    def send_back(slot, who):
        at = rows_at(slot * SLOT, SLOT, SLOT)
        pltpu.make_async_remote_copy(
            src_ref=mean.at[at], dst_ref=ret.at[at], send_sem=ret_send_sem,
            recv_sem=ret_sems.at[slot // plan.unit], device_id=who, device_id_type=MESH_ID,
        ).start()

    pieces = chunk // piece

    def finish_chunk(c):
        for i in range(pieces):
            finish(c * pieces + i)

    def finish_and_send(u):
        finish_chunk(u)
        source.each(u - 1, send_back)

    finish_chunk(0)
    finish_chunk(1)
    for step in range(plane - 1, 0, -1):
        send_near(
            plane - 1 - step, (to.me[0], to.shift(1, step // (ny * nc)), to.shift(2, step // nc % ny), to.shift(3, step % nc))
        )
    source.each(0, send_back)
    plan.loop(2, plan.units, finish_and_send)
    ret[own, :] = mean[own, :]

    near_rows = pl.ds(0, plane - 1)
    pltpu.make_async_copy(near.at[near_rows], near.at[near_rows], dup_sems.at[1]).wait()
    far[pl.ds(0, 1), :] = jnp.sum(near[...], axis=0, keepdims=True)
    source.each(last_unit, send_back)
    for step in range(1, nz):
        pltpu.make_async_remote_copy(
            src_ref=far.at[pl.ds(0, 1)], dst_ref=far.at[pl.ds(step, 1)], send_sem=dup_sems.at[2],
            recv_sem=dup_sems.at[3], device_id=(to.shift(0, step), *to.me[1:]), device_id_type=MESH_ID,
        ).start()

    def add_back(c, last):
        rhs = ret[rows_at(c * chunk, chunk, chunk), :]
        order = wide_line(ord_ref, c, plan)
        own_row = lax.broadcasted_iota(i32, (block, chunk), 0)
        for b in range(rows // block):
            at = pl.ds(b * block, block)
            pick = onehot(own_row == order - b * block)
            total = back[at, :] + jnp.dot(pick, rhs, preferred_element_type=f32)
            if last:
                out_ref[at, :] = total.astype(bf16)
            else:
                back[at, :] = total

    def backs(c):
        wait_chunk(mean, ret, ret_sems, c)
        add_back(c, False)

    plan.loop(0, final, backs)
    far_rows = pl.ds(0, nz - 1)
    pltpu.make_async_copy(far.at[far_rows], far.at[far_rows], dup_sems.at[3]).wait()
    dup_ref[...] = jnp.broadcast_to(jnp.sum(far[...], axis=0, keepdims=True), (8, LANES)).astype(i32)
    wait_chunk(mean, ret, ret_sems, final, True)
    add_back(final, True)
    sent = pl.ds(0, rows - SLOT)
    pltpu.make_async_copy(tag_send.at[others], tag_recv.at[others], tag_sems.at[0]).wait()
    forward.wait_send()
    pltpu.make_async_copy(send.at[sent], recv.at[sent], pay_send_sem).wait()
    pltpu.make_async_copy(mean.at[sent], ret.at[sent], ret_send_sem).wait()
    pltpu.make_async_copy(near.at[near_rows], near.at[near_rows], dup_sems.at[0]).wait()
    pltpu.make_async_copy(far.at[far_rows], far.at[far_rows], dup_sems.at[2]).wait()


def on_device(plan, payload, first_key, second_key, live, first_bucket, second_bucket):
    rows, dev, lines = plan.rows, plan.devices, plan.row_lines
    hbm = pl.BlockSpec(memory_space=pltpu.HBM)
    place = plan.slot_of(first_bucket, second_bucket) * rows + lax.iota(i32, rows)
    columns = (place, jnp.where(live > 0, first_key, -1), second_key)
    tile = lambda n, m, t: pltpu.VMEM((n, m), t)
    group_mean, dups = pl.pallas_call(
        functools.partial(kernel, plan),
        out_shape=(jax.ShapeDtypeStruct((rows, LANES), bf16), jax.ShapeDtypeStruct((8, LANES), i32)),
        in_specs=[hbm] * 4,
        out_specs=(pl.BlockSpec(memory_space=pltpu.VMEM),) * 2,
        scratch_shapes=[
            pltpu.VMEM((3, lines, LANES), i32),
            tile(lines, LANES, i32),
            *[tile(rows, LANES, bf16) for _ in range(5)],
            tile(rows, LANES, i32),
            tile(rows, LANES, i32),
            *[tile(dev // 2, LANES, i32) for _ in range(3)],
            tile(lines, LANES, i32),
            tile(lines, LANES, i32),
            tile(rows, 2 * LANES, f32),
            tile(rows, LANES, f32),
            tile(plan.devices // plan.dims[0], LANES, f32),
            tile(plan.dims[0], LANES, f32),
            pltpu.SemaphoreType.DMA,
            pltpu.SemaphoreType.DMA((4,)),
            pltpu.SemaphoreType.DMA,
            pltpu.SemaphoreType.DMA((plan.units,)),
            pltpu.SemaphoreType.DMA,
            pltpu.SemaphoreType.DMA((plan.units,)),
            pltpu.SemaphoreType.DMA((4,)),
            pltpu.SemaphoreType.DMA((3,)),
        ],
        compiler_params=pltpu.CompilerParams(
            collective_id=0, has_side_effects=True, vmem_limit_bytes=52 * 2**20
        ),
        name="filter",
    )(payload, *[column.reshape(lines, LANES) for column in columns])
    return group_mean, dups[0, 0]


def build(torus, plan):
    rows = P(AXES)
    return jax.shard_map(
        functools.partial(on_device, plan),
        mesh=torus,
        in_specs=(P(AXES, None), rows, rows, rows, rows, rows),
        out_specs=(P(AXES, None), P()),
        check_vma=False,
    )


def solution(mesh):
    dims = (8, 4, 4, 2)
    return build(Mesh(mesh.devices.reshape(dims), AXES), Plan(dims, 1024))
```

```python
import functools

import jax
import jax.numpy as jnp
from jax import lax
from jax.experimental import pallas as pl
from jax.experimental.pallas import tpu as pltpu
from jax.sharding import Mesh
from jax.sharding import PartitionSpec as P

AXES = ("z", "x", "y", "c")
MESH_ID = pl.DeviceIdType.MESH
f32, bf16, i32 = jnp.float32, jnp.bfloat16, jnp.int32
SLOT = 16
LANES = 128


def onehot(mask):
    return jnp.where(mask, 1.0, 0.0).astype(bf16)


def when(condition, act):
    if not isinstance(condition, bool):
        pl.when(condition)(act)
    elif condition:
        act()


def rows_at(start, size, align):
    return pl.ds(pl.multiple_of(start, align), size)


class Plan:
    def __init__(self, dims, block, unrolled=False):
        nz, nx, ny, nc = self.dims = dims
        self.unit = nz * nx
        self.units = ny * nc
        self.devices = self.unit * self.units
        self.rows = self.devices * SLOT
        self.chunk = self.unit * SLOT
        self.block = block
        self.row_lines = self.rows // LANES
        self.unrolled = unrolled
        self.z_steps = [nz // 2]
        for far in range(nz // 2 - 1, 0, -1):
            self.z_steps += [far, nz - far]
        self.z_steps.append(0)

    def loop(self, low, high, body):
        if self.unrolled:
            for i in range(low, high):
                body(i)
        else:
            lax.fori_loop(low, high, lambda i, carry: (body(i), carry)[1], 0)

    def slot_of(self, first_bucket, second_bucket):
        nz, nx, ny, nc = self.dims
        coords = (
            lax.shift_right_logical(first_bucket, nx.bit_length() - 1), first_bucket & (nx - 1),
            lax.shift_right_logical(second_bucket, nc.bit_length() - 1), second_bucket & (nc - 1),
        )
        z, x, y, c = [(at - lax.axis_index(axis)) & (n - 1) for n, axis, at in zip(self.dims, AXES, coords)]
        far = jnp.minimum(z, nz - z)
        z_at = (nz // 2 - 1 - far) * 2 + 1 + jnp.where(z > nz // 2, 1, 0)
        z_at = jnp.where(far == nz // 2, 0, z_at)
        turn = ((y - x) & (ny - 1)) * nc + c
        return (self.units - 1 - turn) * self.unit + z_at * nx + nx - 1 - x


class Partners:
    def __init__(self, plan, sign):
        self.plan, self.sign = plan, sign
        self.me = [lax.axis_index(axis) for axis in AXES]
        self.z = [self.shift(0, step) for step in plan.z_steps]
        self.x = [self.shift(1, step) for step in range(plan.dims[1] - 1, -1, -1)]

    def shift(self, dim, step):
        n = self.plan.dims[dim]
        return lax.rem(self.me[dim] + (step if self.sign > 0 else 2 * n - step), n)

    def each(self, u, act):
        plan = self.plan
        nz, nx, ny, nc = plan.dims
        turn = plan.units - 1 - u
        c = self.shift(3, turn % nc if isinstance(u, int) else lax.rem(turn, nc))
        y_turn = turn // nc if isinstance(u, int) else lax.div(turn, nc)
        y = [self.shift(2, (y_turn + step) % ny if isinstance(u, int) else lax.rem(y_turn + step, ny)) for step in range(nx - 1, -1, -1)]
        for i, z in enumerate(self.z):
            for k, x in enumerate(self.x):
                if isinstance(u, int) and u == plan.units - 1 and i == nz - 1 and k == nx - 1:
                    continue
                act(u * plan.unit + i * nx + k, (z, x, y[k], c))

    def greet(self, barrier):
        plan = self.plan
        nz, nx, ny, nc = plan.dims
        tails = [(self.shift(2, y + ny // 2), self.shift(3, c + 1)) for y in range(ny) for c in range(nc)]
        for i, z in enumerate(self.z):
            for k in range(nx):
                for j, tail in enumerate(tails):
                    own = i == nz - 1 and (k + nx // 2) % nx == 0 and (j // nc + ny // 2) % ny == 0 and (j + 1) % nc == 0
                    if not own:
                        who = (z, self.x[(nx // 2 - 1 - k) % nx], *tail)
                        pl.semaphore_signal(barrier, inc=1, device_id=who, device_id_type=MESH_ID)


def sorted_lines(key, others):
    lines = key.shape[0]
    row, lane = lax.broadcasted_iota(i32, key.shape, 0), lax.broadcasted_iota(i32, key.shape, 1)

    def bit(size):
        at, size = (lane, size) if size < LANES else (row, size // LANES)
        return lax.shift_right_logical(at, size.bit_length() - 1) & 1

    size = 2
    while size <= lines * LANES:
        step = size // 2
        while step:
            upper = bit(step)
            keep_max = upper != bit(size) if size < lines * LANES else upper == 1
            axis, by, span = (1, step, LANES) if step < LANES else (0, step // LANES, lines)

            def other(a, upper=upper, axis=axis, by=by, span=span):
                return jnp.where(upper == 1, pltpu.roll(a, by, axis), pltpu.roll(a, span - by, axis))

            there = other(key)
            new = jnp.where(keep_max, jnp.maximum(key, there), jnp.minimum(key, there))
            moved = new != key
            others = [jnp.where(moved, other(a), a) for a in others]
            key = new
            step //= 2
        size *= 2
    return key, others


def column_form(lines, col_ref, plan):
    turned = jnp.transpose(lines)
    for b in range(plan.row_lines):
        col_ref[pl.ds(b * LANES, LANES), :] = jnp.broadcast_to(turned[:, b : b + 1], (LANES, LANES))


def wide_line(ref, chunk_index, plan):
    n = plan.chunk // LANES
    return jnp.concatenate([ref[pl.ds(chunk_index * n + t, 1), :] for t in range(n)], axis=1)


def kernel(plan, pay_hbm, *refs):
    body(plan, pay_hbm, refs[:3], *refs[3:])


def body(plan, pay_hbm, small, out_ref, dup_ref, fields, ord_ref, pay, send, recv, mean, ret, col_a, col_b,
           tag_send, tag_recv, tag_other, line_a, line_b, acc, back, near, far, io_sem, tag_sems, pay_send_sem, pay_sems,
           ret_send_sem, ret_sems, dup_sems, field_sems):
    dev, rows, chunk, block = plan.devices, plan.rows, plan.chunk, plan.block
    last_unit = plan.units - 1
    to, source = Partners(plan, 1), Partners(plan, -1)
    loads = [pltpu.make_async_copy(ref, fields.at[i], field_sems.at[i]) for i, ref in enumerate(small)]
    load = pltpu.make_async_copy(pay_hbm, pay, io_sem)
    for each in (*loads, load):
        each.start()
    barrier = pltpu.get_barrier_semaphore()
    to.greet(barrier)

    for each in loads:
        each.wait()
    place, (first_key, second_key) = sorted_lines(fields[0], [fields[1], fields[2]])
    order = place & (rows - 1)
    ord_ref[...] = order
    second_key = pltpu.roll(second_key, LANES // 2, 1)

    part = lax.broadcasted_iota(i32, (8, LANES), 1) // SLOT
    sub = lax.broadcasted_iota(i32, (8, LANES), 0)
    spots = [part == lax.rem(sub + q, 8) for q in (0, 4, 2, 6)]
    quarter = LANES // 4
    tagged = [first_key, second_key, pltpu.roll(first_key, quarter, 1), pltpu.roll(second_key, quarter, 1)]
    unit_lines = plan.unit // 8
    pairs_of_units = plan.units // 2
    for v in range(pairs_of_units):
        for i in range(unit_lines):
            other, like = 2 * v * unit_lines + i, (2 * v + 1) * unit_lines + i
            one, two, three, four = [
                jnp.broadcast_to(keys[at : at + 1, :], (8, LANES)) for keys, at in zip(tagged, (like, like, other, other))
            ]
            line = jnp.where(spots[0], one, jnp.where(spots[1], two, jnp.where(spots[2], three, four)))
            tag_send[pl.ds(v * plan.unit + 8 * i, 8), :] = line
    column_form(order, col_a, plan)
    load.wait()

    deep = min(1024, rows)
    lane = lax.broadcasted_iota(i32, (chunk, deep), 1)

    def permute(c):
        at = rows_at(c * chunk, chunk, chunk)
        want = jnp.concatenate([col_a[at, :]] * (deep // LANES), axis=1)
        total = jnp.zeros((chunk, LANES), f32)
        for k in range(rows // deep):
            pick = onehot(want - k * deep == lane)
            total = total + jnp.dot(pick, pay[pl.ds(k * deep, deep), :], preferred_element_type=f32)
        send[at, :] = total.astype(bf16)

    def send_tags(v):
        def send_tag(slot, who):
            at = pl.ds(slot - plan.unit * (v + 1), 1)
            pltpu.make_async_remote_copy(
                src_ref=tag_send.at[at], dst_ref=tag_recv.at[at], send_sem=tag_sems.at[0], recv_sem=tag_sems.at[1],
                device_id=who, device_id_type=MESH_ID,
            ).start()

        to.each(2 * v + 1, send_tag)

    def send_row(slot, who):
        at = rows_at(slot * SLOT, SLOT, SLOT)
        pltpu.make_async_remote_copy(
            src_ref=send.at[at], dst_ref=recv.at[at], send_sem=pay_send_sem,
            recv_sem=pay_sems.at[slot // plan.unit], device_id=who, device_id_type=MESH_ID,
        ).start()

    pl.semaphore_wait(barrier, dev - 1)
    plan.loop(0, pairs_of_units // 2, send_tags)

    lines = dev // 2
    others, own_line = pl.ds(0, lines - 1), pl.ds(lines - 1, 1)
    tag_recv[own_line, :] = tag_send[own_line, :]
    forward = pltpu.make_async_remote_copy(
        src_ref=tag_recv, dst_ref=tag_other, send_sem=tag_sems.at[2], recv_sem=tag_sems.at[3],
        device_id=(*to.me[:3], to.shift(3, 1)), device_id_type=MESH_ID,
    )

    def hand_on():
        pltpu.make_async_copy(tag_send.at[others], tag_recv.at[others], tag_sems.at[1]).wait()
        forward.start()

    def first_sent():
        plan.loop(pairs_of_units // 2, pairs_of_units - 1, send_tags)
        send_tags(pairs_of_units - 1)
        to.each(0, send_row)

    def permute_and_send(u):
        permute(u)
        when(u == 0, first_sent)
        when(u >= 2, lambda: to.each(u - 1, send_row))
        when(u == last_unit - 1, hand_on)

    plan.loop(0, plan.units, permute_and_send)
    own = pl.ds(rows - SLOT, SLOT)
    recv[own, :] = send[own, :]
    to.each(last_unit, send_row)
    acc[...] = jnp.zeros_like(acc)

    def take(ref, v, i, line, at, by):
        got = ref[pl.ds(v * plan.unit + 8 * i, 8), :]
        one, two = [jnp.sum(jnp.where(spot, got, 0), axis=0, keepdims=True) for spot in spots[at : at + 2]]
        line_a[pl.ds(line, 1), :] = pltpu.roll(one, by, 1) if by else one
        line_b[pl.ds(line, 1), :] = pltpu.roll(two, (LANES // 2 + by) % LANES, 1)

    for v in range(pairs_of_units):
        for i in range(unit_lines):
            take(tag_recv, v, i, (2 * v + 1) * unit_lines + i, 0, 0)
    forward.wait_recv()
    for v in range(pairs_of_units):
        for i in range(unit_lines):
            take(tag_other, v, i, 2 * v * unit_lines + i, 2, LANES - quarter)
    column_form(line_a[...], col_a, plan)
    column_form(line_b[...], col_b, plan)
    keys = line_a[...]
    line_a[...] = jnp.where(keys < 0, -2, keys)

    def wait_chunk(src, dst, sems, c, last=False):
        at = pl.ds(0, chunk - SLOT if last else chunk)
        pltpu.make_async_copy(src.at[at], dst.at[at], sems.at[c]).wait()

    def add_pairs(c):
        rhs = jnp.concatenate([recv[rows_at(c * chunk, chunk, chunk), :], jnp.ones((chunk, LANES), bf16)], axis=1)
        one, two = wide_line(line_a, c, plan), wide_line(line_b, c, plan)
        for b in range(rows // block):
            at = pl.ds(b * block, block)
            col_one = jnp.concatenate([col_a[at, :]] * (chunk // LANES), axis=1)
            col_two = jnp.concatenate([col_b[at, :]] * (chunk // LANES), axis=1)
            same = onehot((col_one == one) & (col_two == two))
            acc[at, :] += jnp.dot(same, rhs, preferred_element_type=f32)

    final = last_unit

    def pairs(c):
        wait_chunk(send, recv, pay_sems, c)
        add_pairs(c)

    plan.loop(0, final, pairs)
    wait_chunk(send, recv, pay_sems, final, True)
    add_pairs(final)

    piece = min(256, chunk)
    nz, nx, ny, nc = plan.dims
    plane = nx * ny * nc
    own_near = pl.ds(plane - 1, 1)

    def counts(p, dups):
        at = rows_at(p * piece, piece, piece)
        count = acc[at, pl.ds(LANES, LANES)]
        inverse = 1.0 / jnp.maximum(count, 1.0)
        acc[at, pl.ds(LANES, LANES)] = inverse
        again = jnp.where(count > 0.0, 1.0 - inverse, 0.0)
        return dups + jnp.sum(again.reshape(piece // 8, 8, LANES), axis=0)

    dups = lax.fori_loop(0, rows // piece, counts, jnp.zeros((8, LANES), f32))
    near[own_near, :] = jnp.floor(jnp.sum(dups, axis=0, keepdims=True) + 0.5)

    def finish(p):
        at = rows_at(p * piece, piece, piece)
        mean[at, :] = (acc[at, pl.ds(0, LANES)] * acc[at, pl.ds(LANES, LANES)]).astype(bf16)

    def send_near(step, who):
        pltpu.make_async_remote_copy(
            src_ref=near.at[own_near], dst_ref=near.at[pl.ds(step, 1)], send_sem=dup_sems.at[0],
            recv_sem=dup_sems.at[1], device_id=who, device_id_type=MESH_ID,
        ).start()

    def send_back(slot, who):
        at = rows_at(slot * SLOT, SLOT, SLOT)
        pltpu.make_async_remote_copy(
            src_ref=mean.at[at], dst_ref=ret.at[at], send_sem=ret_send_sem,
            recv_sem=ret_sems.at[slot // plan.unit], device_id=who, device_id_type=MESH_ID,
        ).start()

    pieces = chunk // piece

    def finish_chunk(c):
        for i in range(pieces):
            finish(c * pieces + i)

    def finish_and_send(u):
        finish_chunk(u)
        source.each(u - 1, send_back)

    finish_chunk(0)
    finish_chunk(1)
    for step in range(plane - 1, 0, -1):
        send_near(
            plane - 1 - step, (to.me[0], to.shift(1, step // (ny * nc)), to.shift(2, step // nc % ny), to.shift(3, step % nc))
        )
    source.each(0, send_back)
    plan.loop(2, plan.units, finish_and_send)
    ret[own, :] = mean[own, :]

    near_rows = pl.ds(0, plane - 1)
    pltpu.make_async_copy(near.at[near_rows], near.at[near_rows], dup_sems.at[1]).wait()
    far[pl.ds(0, 1), :] = jnp.sum(near[...], axis=0, keepdims=True)
    source.each(last_unit, send_back)
    for step in range(1, nz):
        pltpu.make_async_remote_copy(
            src_ref=far.at[pl.ds(0, 1)], dst_ref=far.at[pl.ds(step, 1)], send_sem=dup_sems.at[2],
            recv_sem=dup_sems.at[3], device_id=(to.shift(0, step), *to.me[1:]), device_id_type=MESH_ID,
        ).start()

    def add_back(c, last):
        rhs = ret[rows_at(c * chunk, chunk, chunk), :]
        order = wide_line(ord_ref, c, plan)
        own_row = lax.broadcasted_iota(i32, (block, chunk), 0)
        for b in range(rows // block):
            at = pl.ds(b * block, block)
            pick = onehot(own_row == order - b * block)
            total = back[at, :] + jnp.dot(pick, rhs, preferred_element_type=f32)
            if last:
                out_ref[at, :] = total.astype(bf16)
            else:
                back[at, :] = total

    def backs(c):
        wait_chunk(mean, ret, ret_sems, c)
        add_back(c, False)

    back[...] = jnp.zeros_like(back)
    plan.loop(0, final, backs)
    far_rows = pl.ds(0, nz - 1)
    pltpu.make_async_copy(far.at[far_rows], far.at[far_rows], dup_sems.at[3]).wait()
    dup_ref[...] = jnp.broadcast_to(jnp.sum(far[...], axis=0, keepdims=True), (8, LANES)).astype(i32)
    wait_chunk(mean, ret, ret_sems, final, True)
    add_back(final, True)
    sent = pl.ds(0, rows - SLOT)
    pltpu.make_async_copy(tag_send.at[others], tag_recv.at[others], tag_sems.at[0]).wait()
    forward.wait_send()
    pltpu.make_async_copy(send.at[sent], recv.at[sent], pay_send_sem).wait()
    pltpu.make_async_copy(mean.at[sent], ret.at[sent], ret_send_sem).wait()
    pltpu.make_async_copy(near.at[near_rows], near.at[near_rows], dup_sems.at[0]).wait()
    pltpu.make_async_copy(far.at[far_rows], far.at[far_rows], dup_sems.at[2]).wait()


def on_device(plan, payload, first_key, second_key, live, first_bucket, second_bucket):
    rows, dev, lines = plan.rows, plan.devices, plan.row_lines
    hbm = pl.BlockSpec(memory_space=pltpu.HBM)
    place = plan.slot_of(first_bucket, second_bucket) * rows + lax.iota(i32, rows)
    columns = (place, jnp.where(live > 0, first_key, -1), second_key)
    tile = lambda n, m, t: pltpu.VMEM((n, m), t)
    group_mean, dups = pl.pallas_call(
        functools.partial(kernel, plan),
        out_shape=(jax.ShapeDtypeStruct((rows, LANES), bf16), jax.ShapeDtypeStruct((8, LANES), i32)),
        in_specs=[hbm] * 4,
        out_specs=(pl.BlockSpec(memory_space=pltpu.VMEM),) * 2,
        scratch_shapes=[
            pltpu.VMEM((3, lines, LANES), i32),
            tile(lines, LANES, i32),
            *[tile(rows, LANES, bf16) for _ in range(5)],
            tile(rows, LANES, i32),
            tile(rows, LANES, i32),
            *[tile(dev // 2, LANES, i32) for _ in range(3)],
            tile(lines, LANES, i32),
            tile(lines, LANES, i32),
            tile(rows, 2 * LANES, f32),
            tile(rows, LANES, f32),
            tile(plan.devices // plan.dims[0], LANES, f32),
            tile(plan.dims[0], LANES, f32),
            pltpu.SemaphoreType.DMA,
            pltpu.SemaphoreType.DMA((4,)),
            pltpu.SemaphoreType.DMA,
            pltpu.SemaphoreType.DMA((plan.units,)),
            pltpu.SemaphoreType.DMA,
            pltpu.SemaphoreType.DMA((plan.units,)),
            pltpu.SemaphoreType.DMA((4,)),
            pltpu.SemaphoreType.DMA((3,)),
        ],
        compiler_params=pltpu.CompilerParams(
            collective_id=0, has_side_effects=True, vmem_limit_bytes=52 * 2**20
        ),
        name="filter",
    )(payload, *[column.reshape(lines, LANES) for column in columns])
    return group_mean, dups[0, 0]


def build(torus, plan):
    rows = P(AXES)
    return jax.shard_map(
        functools.partial(on_device, plan),
        mesh=torus,
        in_specs=(P(AXES, None), rows, rows, rows, rows, rows),
        out_specs=(P(AXES, None), P()),
        check_vma=False,
    )


def solution(mesh):
    dims = (8, 4, 4, 2)
    return build(Mesh(mesh.devices.reshape(dims), AXES), Plan(dims, 1024))
```
